32 devices in a mesh: lon: 8 (over z, x), lat: 4 (over y, core).
Axes of the slice: x: 2, y: 2, z: 4, core: 2. Of those that a mesh axis runs over, the one named last changes fastest.
Arguments:
- tracers: float32 [40, 8, 32, 1024], P(None, None, 'lat', 'lon'), may hold values from -6 to 6
- kmt: int32 [32, 1024], P('lat', 'lon'), may hold values from 0 to 8
Outputs:
- updated: float32 [40, 8, 32, 1024], P(None, None, 'lat', 'lon')
The draws below stay inside these ranges and needn't reach their ends.
Inputs may be any that keep to these rules, and one draw needn't show every extreme that they name: Level k of column (j, i) is ocean exactly when k < kmt[j, i].
All inputs are finite; a program needn't handle non-finite values.
Results may differ from the reference program's by a relative error of at most 0.00002.
Values sent between devices are 32-bit elements; how exact they have to be, the bound alone decides.
A program may use at most 64 MiB of HBM per device.

```python
import jax
import jax.numpy as jnp
from jax import lax

NTRAC = 40
NZ = 8
NY = 32
NX = 1024


def with_ends(array, rng, least, largest):
    longest = array.shape.index(max(array.shape))
    spots = []
    for shift in (0, 1):
        where = [jax.random.randint(jax.random.fold_in(rng, axis), (), 0, length) for axis, length in enumerate(array.shape)]
        where[longest] = (where[longest] + shift) % array.shape[longest]
        spots.append(tuple(where))
    return array.at[spots[0]].set(least).at[spots[1]].set(largest)


def block_scale(key, extent, pieces, least, largest):
    level, own = 1.0, jax.random.fold_in(key, 6)
    for dim, blocks in pieces:
        heights = jnp.exp(jax.random.uniform(jax.random.fold_in(own, dim), (blocks,), jnp.float32, least / len(pieces), largest / len(pieces)))
        level = level * jnp.repeat(heights, extent[dim] // blocks).reshape([-1 if axis == dim else 1 for axis in range(len(extent))])
    return level


def normal_values(rng, dims, scale, bound, pieces=(), kind=jnp.bfloat16):
    level = block_scale(rng, dims, pieces, -0.22, 0.18) if pieces else 1.0
    values = jax.random.normal(rng, dims, jnp.float32) * scale * level
    return jnp.minimum(jnp.maximum(values, -bound), bound).astype(kind)


def setup_inputs(seed: int = 0) -> dict:
    streams_of = jax.random.split(jax.random.key(seed), 3)
    tracers = normal_values(streams_of[0], (NTRAC, NZ, NY, NX), 1.0, 6.0, ((2, 4), (3, 8)), jnp.float32)
    kmt = with_ends(jax.random.randint(streams_of[1], (NY, NX), 0, NZ + 1), jax.random.fold_in(streams_of[1], 1), 0, NZ).astype(jnp.int32)
    return dict(tracers=tracers, kmt=kmt)


THERMAL = 0.2
HALINE = 0.8
REDI_COEF = 0.1
SKEW_COEF = 0.05
SLOPE_MAX = 0.6
SLOPE_WIDTH = 0.2


def taper(slope):
    return slope * 0.5 * (1.0 + jnp.tanh((SLOPE_MAX - jnp.abs(slope)) / SLOPE_WIDTH))


def pad_levels(values):
    zero_layer = jnp.zeros_like(values[..., :1, :, :])
    return jnp.concatenate([zero_layer, values, zero_layer], axis=-3)


def slope_fields(density, wet_mask):
    level_mask = wet_mask[1:] * wet_mask[:-1]
    strat = (density[1:] - density[:-1]) * level_mask
    strat_pad = pad_levels(strat)
    strat_cell = 0.5 * (strat_pad[:-1] + strat_pad[1:])
    east_mask = wet_mask[:, 1:-1, :-1] * wet_mask[:, 1:-1, 1:]
    north_mask = wet_mask[:, :-1, 1:-1] * wet_mask[:, 1:, 1:-1]
    grad_east = (density[:, 1:-1, 1:] - density[:, 1:-1, :-1]) * east_mask
    strat_east = 0.5 * (strat_cell[:, 1:-1, 1:] + strat_cell[:, 1:-1, :-1])
    slope_x = taper(grad_east / jnp.maximum(strat_east, 1.0))
    grad_north = (density[:, 1:, 1:-1] - density[:, :-1, 1:-1]) * north_mask
    strat_north = 0.5 * (strat_cell[:, 1:, 1:-1] + strat_cell[:, :-1, 1:-1])
    slope_y = taper(grad_north / jnp.maximum(strat_north, 1.0))
    cell_x = 0.5 * (slope_x[..., :-1] + slope_x[..., 1:])
    cell_y = 0.5 * (slope_y[:, :-1, :] + slope_y[:, 1:, :])
    level_x = 0.5 * (cell_x[:-1] + cell_x[1:])
    level_y = 0.5 * (cell_y[:-1] + cell_y[1:])
    return (level_mask, east_mask, north_mask, slope_x, slope_y, level_x, level_y)


def tracer_step(field, fields):
    level_mask, east_mask, north_mask, slope_x, slope_y, level_x, level_y = fields
    vert_diff = (field[..., 1:, :, :] - field[..., :-1, :, :]) * level_mask
    vert_pad = pad_levels(vert_diff)
    vert_cell = 0.5 * (vert_pad[..., :-1, :, :] + vert_pad[..., 1:, :, :])
    grad_x = (field[..., 1:-1, 1:] - field[..., 1:-1, :-1]) * east_mask
    grad_y = (field[..., 1:, 1:-1] - field[..., :-1, 1:-1]) * north_mask
    flux_x = -(REDI_COEF * grad_x + (REDI_COEF - SKEW_COEF) * slope_x
               * 0.5 * (vert_cell[..., 1:-1, 1:] + vert_cell[..., 1:-1, :-1])) * east_mask
    flux_y = -(REDI_COEF * grad_y + (REDI_COEF - SKEW_COEF) * slope_y
               * 0.5 * (vert_cell[..., 1:, 1:-1] + vert_cell[..., :-1, 1:-1])) * north_mask
    cell_gx = 0.5 * (grad_x[..., :-1] + grad_x[..., 1:])
    cell_gy = 0.5 * (grad_y[..., :-1, :] + grad_y[..., 1:, :])
    level_gx = 0.5 * (cell_gx[..., :-1, :, :] + cell_gx[..., 1:, :, :])
    level_gy = 0.5 * (cell_gy[..., :-1, :, :] + cell_gy[..., 1:, :, :])
    flux_z = -((REDI_COEF + SKEW_COEF) * (level_x * level_gx + level_y * level_gy)
               + REDI_COEF * (level_x * level_x + level_y * level_y) * vert_diff[..., 1:-1, 1:-1]) * level_mask[:, 1:-1, 1:-1]
    flux_pad = pad_levels(flux_z)
    tendency = -((flux_x[..., 1:] - flux_x[..., :-1]) + (flux_y[..., 1:, :] - flux_y[..., :-1, :])
                 + (flux_pad[..., 1:, :, :] - flux_pad[..., :-1, :, :]))
    return field[..., 1:-1, 1:-1] + tendency


def extend(field):
    beside_all = jnp.concatenate([field[..., -1:], field, field[..., :1]], axis=-1)
    north_row = beside_all[..., -1:, ::-1]
    south_row = jnp.zeros_like(beside_all[..., :1, :])
    return jnp.concatenate([south_row, beside_all, north_row], axis=-2)


def reference(tracers, kmt):
    level_index = lax.broadcasted_iota(jnp.int32, (NZ, NY, NX), 0)
    wet_mask = (level_index < kmt[None]).astype(jnp.float32)
    density = HALINE * tracers[1] - THERMAL * tracers[0]
    fields = slope_fields(extend(density), extend(wet_mask))
    return lax.map(lambda single: tracer_step(extend(single), fields), tracers)
```

```python
import functools

import jax
import jax.numpy as jnp
from jax import lax
from jax.experimental import pallas as pl
from jax.experimental.pallas import tpu as pltpu
from jax.sharding import PartitionSpec as P

THERMAL = 0.2
HALINE = 0.8
REDI = 0.1
SKEW = 0.05
SLOPE_MAX = 0.6
SLOPE_WIDTH = 0.2

MESH = pl.DeviceIdType.MESH
PAD = 8
HEAD = 8
PIECES = 5
C, E, W, N, S = range(5)


def taper(slope):
    return slope * 0.5 * (1.0 + jnp.tanh((SLOPE_MAX - jnp.abs(slope)) / SLOPE_WIDTH))


def shift_sum(values, k):
    above = values[k - 1] if k > 0 else None
    below = values[k] if k < len(values) else None
    return above, below


def total(*terms):
    terms = [term for term in terms if term is not None]
    result = terms[0]
    for term in terms[1:]:
        result = result + term
    return result


def coefficients(rho, kmt, levels):
    zero = jnp.zeros_like(kmt[C])
    wet, lm, cell = [], [], []
    for d in range(5):
        w = [(kmt[d] > float(k)).astype(jnp.float32) for k in range(levels)]
        m = [w[k + 1] * w[k] for k in range(levels - 1)]
        st = [(rho[d][k + 1] - rho[d][k]) * m[k] for k in range(levels - 1)]
        wet.append(w)
        lm.append(m)
        cell.append([0.5 * total(*shift_sum(st, k)) for k in range(levels)])
    mask = [None] + [[wet[C][k] * wet[d][k] for k in range(levels)] for d in (E, W, N, S)]
    slope = [None]
    for d in (E, W, N, S):
        sign = 1.0 if d in (E, N) else -1.0
        slope.append(
            [
                taper(
                    sign
                    * (rho[d][k] - rho[C][k])
                    * mask[d][k]
                    / jnp.maximum(0.5 * (cell[d][k] + cell[C][k]), 1.0)
                )
                for k in range(levels)
            ]
        )
    cx = [0.5 * (slope[W][k] + slope[E][k]) for k in range(levels)]
    cy = [0.5 * (slope[S][k] + slope[N][k]) for k in range(levels)]
    xs, ys, zs = [], [], []
    for k in range(levels - 1):
        sxw = 0.5 * (cx[k] + cx[k + 1])
        syw = 0.5 * (cy[k] + cy[k + 1])
        xs.append(((REDI + SKEW) * 0.25) * sxw * lm[C][k])
        ys.append(((REDI + SKEW) * 0.25) * syw * lm[C][k])
        zs.append(REDI * (sxw * sxw + syw * syw) * lm[C][k])
    out = {}
    for k in range(levels):
        first, last = k == 0, k == levels - 1
        centre, up, down = 1.0, zero, zero
        q = zero
        for d in (E, W, N, S):
            sign = 1.0 if d in (E, N) else -1.0
            face = xs if d in (E, W) else ys
            p = (sign * (REDI - SKEW) * 0.25) * slope[d][k] * mask[d][k]
            q = q + p
            lo = zero if first else lm[d][k - 1]
            hi = zero if last else lm[d][k]
            flo = zero if first else face[k - 1]
            fhi = zero if last else face[k]
            own = sign * mask[d][k] * (fhi - flo)
            out[d, k, 1] = REDI * mask[d][k] + p * (lo - hi) + own
            out[d, k, 2] = zero if last else p * hi + sign * mask[d][k + 1] * fhi
            out[d, k, 0] = zero if first else -p * lo - sign * mask[d][k - 1] * flo
            centre = centre - REDI * mask[d][k] - own
            if not last:
                up = up - sign * mask[d][k + 1] * fhi
            if not first:
                down = down + sign * mask[d][k - 1] * flo
        lo = zero if first else lm[C][k - 1]
        hi = zero if last else lm[C][k]
        zlo = zero if first else zs[k - 1]
        zhi = zero if last else zs[k]
        out[C, k, 1] = centre + q * (lo - hi) - (zhi + zlo)
        out[C, k, 2] = up + q * hi + zhi
        out[C, k, 0] = down - q * lo + zlo
    return out


def kernel(
    sizes, x_ref, kmt_ref, out_ref,
    xv, coef, edge, cols, west, east, merged, north, south, from_n, from_s,
    load_sem, send_sem, recv_sem,
):
    tracers, levels, rows, lanes, n_lon, n_lat = sizes
    lon, lat = lax.axis_index("lon"), lax.axis_index("lat")
    at_top = lat == n_lat - 1
    inner = lat > 0
    e_dev = (lax.rem(lon + 1, n_lon), lat)
    w_dev = (lax.rem(lon + n_lon - 1, n_lon), lat)
    fold_dev = (n_lon - 1 - lon, lat)
    plane = levels * rows
    per_reg = lanes // 2

    barrier = pltpu.get_barrier_semaphore()

    def greet(dev):
        pl.semaphore_signal(barrier, inc=1, device_id=dev, device_id_type=MESH)

    @pl.when(at_top)
    def _():
        greet(fold_dev)

    @pl.when(jnp.logical_not(at_top))
    def _():
        greet((lon, lat + 1))

    greet(e_dev)
    greet(w_dev)

    @pl.when(inner)
    def _():
        greet((lon, lat - 1))

    step = tracers // PIECES * plane
    loads = []
    for i in range(PIECES):
        copy = pltpu.make_async_copy(
            x_ref.at[pl.ds(i * step, step)], xv.at[pl.ds(PAD + i * step, step)], load_sem.at[i]
        )
        copy.start()
        loads.append(copy)

    zeros = jnp.zeros((8, lanes), jnp.float32)
    xv[pl.ds(0, PAD), :] = zeros
    xv[pl.ds(PAD + tracers * plane, PAD), :] = zeros
    lane = lax.broadcasted_iota(jnp.int32, (8, lanes), 1)
    row = lax.broadcasted_iota(jnp.int32, (8, lanes), 0)
    half = lane // 2
    even = lane % 2 == 0

    kmt_own = kmt_ref[...].astype(jnp.float32)
    north[pl.ds(0, HEAD), :] = jnp.broadcast_to(kmt_own[rows - 1 : rows, :], (HEAD, lanes))
    south[pl.ds(0, HEAD), :] = jnp.broadcast_to(kmt_own[0:1, :], (HEAD, lanes))
    regs = tracers * levels // per_reg
    cols[pl.ds(regs * 8, 8), :] = pltpu.roll(kmt_own, 1, 1)

    group = per_reg // levels
    per_piece = tracers // PIECES
    for i in range(PIECES):
        loads[i].wait()

        @pl.loop(i * per_piece, (i + 1) * per_piece)
        def _(t):
            base = PAD + t * plane
            north[pl.ds(HEAD + t * levels, levels), :] = xv[pl.ds(base + rows - 1, levels, stride=rows), :]
            south[pl.ds(HEAD + t * levels, levels), :] = xv[pl.ds(base, levels, stride=rows), :]

        for v in range(i * per_piece // group, (i + 1) * per_piece // group):
            acc = zeros
            for q in range(per_reg):
                value = xv[pl.ds(PAD + (v * per_reg + q) * rows, rows), :]
                acc = jnp.where(half == q, pltpu.roll(value, (2 * q + 1) % lanes, 1), acc)
            cols[pl.ds(v * 8, 8), :] = acc

    @pl.when(inner)
    def _():
        pl.semaphore_wait(barrier, 4)

    @pl.when(jnp.logical_not(inner))
    def _():
        pl.semaphore_wait(barrier, 3)

    small = HEAD + 2 * levels
    big = (tracers - 2) * levels

    def send(src, dst, rows_at, count, s, r, dev):
        return pltpu.make_async_remote_copy(
            src_ref=src.at[pl.ds(rows_at, count)],
            dst_ref=dst.at[pl.ds(rows_at, count)],
            send_sem=send_sem.at[s],
            recv_sem=recv_sem.at[r],
            device_id=dev,
            device_id_type=MESH,
        )

    everything = (regs + 1) * 8
    fold = [send(north, from_n, 0, small, 0, 0, fold_dev), send(north, from_n, small, big, 1, 1, fold_dev)]
    to_n = [send(north, from_s, 0, small, 0, 2, (lon, lat + 1)), send(north, from_s, small, big, 1, 3, (lon, lat + 1))]
    to_s = [send(south, from_n, 0, small, 2, 0, (lon, lat - 1)), send(south, from_n, small, big, 3, 1, (lon, lat - 1))]
    to_e = send(cols, west, 0, everything, 4, 4, e_dev)
    to_w = send(cols, east, 0, everything, 5, 5, w_dev)
    for part in range(2):

        @pl.when(at_top)
        def _():
            fold[part].start()

        @pl.when(jnp.logical_not(at_top))
        def _():
            to_n[part].start()

        @pl.when(inner)
        def _():
            to_s[part].start()

        if part == 0:
            to_e.start()
            to_w.start()

    @pl.when(jnp.logical_not(inner))
    def _():
        for i in range(small // 8):
            from_s[pl.ds(i * 8, 8), :] = zeros

    to_e.wait_recv()
    to_w.wait_recv()
    for v in range(regs + 1):
        merged[pl.ds(v * 8, 8), :] = jnp.where(even, west[pl.ds(v * 8, 8), :], east[pl.ds(v * 8, 8), :])

    def beside(value, halo, shift):
        m = pltpu.roll(halo, shift, 1)
        e = pltpu.roll(jnp.where(lane == 0, m, value), lanes - 1, 1)
        w = pltpu.roll(jnp.where(lane == lanes - 1, m, value), 1, 1)
        return e, w

    def flipped(value):
        turned = jnp.take_along_axis(value, lanes - 1 - lane, axis=1)
        return jnp.where(at_top, turned, value)

    fold[0].wait_recv()

    @pl.when(inner)
    def _():
        to_n[0].wait_recv()

    rho = [[], [], [], [], []]
    rho_n = flipped(
        HALINE * from_n[pl.ds(HEAD + levels, levels), :] - THERMAL * from_n[pl.ds(HEAD, levels), :]
    )
    rho_s = HALINE * from_s[pl.ds(HEAD + levels, levels), :] - THERMAL * from_s[pl.ds(HEAD, levels), :]
    rho_h = HALINE * pltpu.roll(merged[pl.ds(0, 8), :], lanes - 2 * levels, 1) - THERMAL * merged[pl.ds(0, 8), :]

    def north_of(value, halo):
        return jnp.where(row == rows - 1, halo, pltpu.roll(value, rows - 1, 0))

    def south_of(value, halo):
        return jnp.where(row == 0, halo, pltpu.roll(value, 1, 0))

    for k in range(levels):
        own = HALINE * xv[pl.ds(PAD + plane + k * rows, rows), :] - THERMAL * xv[pl.ds(PAD + k * rows, rows), :]
        e, w = beside(own, rho_h, (lanes - (2 * k + 1)) % lanes)
        rho[C].append(own)
        rho[E].append(e)
        rho[W].append(w)
        rho[N].append(north_of(own, jnp.broadcast_to(rho_n[k : k + 1, :], (rows, lanes))))
        rho[S].append(south_of(own, jnp.broadcast_to(rho_s[k : k + 1, :], (rows, lanes))))
    kmt_e, kmt_w = beside(kmt_own, merged[pl.ds(regs * 8, 8), :], lanes - 1)
    kmts = [
        kmt_own, kmt_e, kmt_w,
        north_of(kmt_own, flipped(from_n[pl.ds(0, 8), :])),
        south_of(kmt_own, from_s[pl.ds(0, 8), :]),
    ]
    table = coefficients(rho, kmts, levels)
    for (d, k, dk), value in table.items():
        coef[pl.ds(((d * 3 + dk) * levels + k) * 8, 8), :] = value
    for slot, (d, at) in enumerate(((N, rows - 1), (S, 0))):
        for dk in range(3):
            place = pl.ds((d * 3 + dk) * plane + at, levels, stride=rows)
            edge[pl.ds((slot * 3 + dk) * 8, 8), :] = coef[place, :]
            coef[place, :] = zeros

    def piece(d, dk, k):
        return coef[pl.ds(((d * 3 + dk) * levels + k) * 8, 8), :]

    together = 2

    @pl.loop(0, tracers // together)
    def _(pair):
        fields = []
        for u in range(together):
            t = pair * together + u
            base = PAD + t * plane
            p0 = t * levels
            reg = merged[pl.ds(pl.multiple_of(p0 // per_reg * 8, 8), 8), :]
            reg = pltpu.roll(reg, lax.rem(lanes - 2 * lax.rem(p0, per_reg) - 1 + lanes, lanes), 1)
            field = []
            for k in range(levels):
                own = xv[pl.ds(pl.multiple_of(base + k * rows, 8), rows), :]
                e, w = beside(own, reg, (lanes - 2 * k) % lanes)
                n = pltpu.roll(own, rows - 1, 0)
                s = pltpu.roll(own, 1, 0)
                field.append((own, e, w, n, s))
            fields.append(field)
        for k in range(levels):
            sums = [None] * together
            for d in range(5):
                for dk in range(3):
                    if not 0 <= k + dk - 1 < levels:
                        continue
                    c = piece(d, dk, k)
                    for u in range(together):
                        term = c * fields[u][k + dk - 1][d]
                        sums[u] = term if sums[u] is None else sums[u] + term
            for u in range(together):
                t = pair * together + u
                out_ref[pl.ds(pl.multiple_of(t * plane + k * rows, 8), rows), :] = sums[u]

    def fix(slot, source, at, turn):
        cs = [edge[pl.ds((slot * 3 + dk) * 8, 8), :] for dk in range(3)]

        @pl.loop(0, tracers, unroll=4)
        def _(t):
            h = source[pl.ds(pl.multiple_of(HEAD + t * levels, 8), levels), :]
            if turn:
                h = flipped(h)
            add = cs[1] * h + cs[2] * pltpu.roll(h, levels - 1, 0) + cs[0] * pltpu.roll(h, 1, 0)
            place = pl.ds(t * plane + at, levels, stride=rows)
            out_ref[place, :] = out_ref[place, :] + add

    @pl.when(inner)
    def _():
        to_n[1].wait_recv()
        fix(1, from_s, 0, False)

    fold[1].wait_recv()
    fix(0, from_n, rows - 1, True)

    for part in range(2):
        fold[part].wait_send()

        @pl.when(inner)
        def _():
            to_s[part].wait_send()

    to_e.wait_send()
    to_w.wait_send()


def solution(mesh):
    n_lon, n_lat = mesh.shape["lon"], mesh.shape["lat"]

    def local(tracers, kmt):
        nt, levels, rows, lanes = tracers.shape
        flat = tracers.reshape(nt * levels * rows, lanes)
        total_rows = nt * levels * rows
        packed = (nt * levels * 2 // lanes + 1) * 8
        halo = HEAD + nt * levels

        def vmem(*shape):
            return pltpu.VMEM(shape, jnp.float32)

        out = pl.pallas_call(
            functools.partial(kernel, (nt, levels, rows, lanes, n_lon, n_lat)),
            out_shape=jax.ShapeDtypeStruct((total_rows, lanes), jnp.float32),
            in_specs=[pl.BlockSpec(memory_space=pl.ANY), pl.BlockSpec(memory_space=pltpu.VMEM)],
            out_specs=pl.BlockSpec(memory_space=pltpu.VMEM),
            scratch_shapes=[
                vmem(total_rows + 2 * PAD, lanes),
                vmem(15 * levels * 8, lanes),
                vmem(6 * 8, lanes),
                vmem(packed, lanes),
                vmem(packed, lanes),
                vmem(packed, lanes),
                vmem(packed, lanes),
                vmem(halo, lanes),
                vmem(halo, lanes),
                vmem(halo, lanes),
                vmem(halo, lanes),
                pltpu.SemaphoreType.DMA((PIECES,)),
                pltpu.SemaphoreType.DMA((6,)),
                pltpu.SemaphoreType.DMA((6,)),
            ],
            compiler_params=pltpu.CompilerParams(collective_id=0, has_side_effects=True),
        )(flat, kmt)
        return out.reshape(nt, levels, rows, lanes)

    return jax.shard_map(
        local,
        mesh=mesh,
        in_specs=(P(None, None, "lat", "lon"), P("lat", "lon")),
        out_specs=P(None, None, "lat", "lon"),
        check_vma=False,
    )
```

```python
import functools

import jax
import jax.numpy as jnp
from jax import lax
from jax.experimental import pallas as pl
from jax.experimental.pallas import tpu as pltpu
from jax.sharding import PartitionSpec as P

THERMAL = 0.2
HALINE = 0.8
REDI = 0.1
SKEW = 0.05
SLOPE_MAX = 0.6
SLOPE_WIDTH = 0.2

MESH = pl.DeviceIdType.MESH
PAD = 8
HEAD = 8
TOGETHER = 2
UNALIGNED = False
C, E, W, N, S = range(5)


def taper(slope):
    return slope * 0.5 * (1.0 + jnp.tanh((SLOPE_MAX - jnp.abs(slope)) / SLOPE_WIDTH))


def shift_sum(values, k):
    above = values[k - 1] if k > 0 else None
    below = values[k] if k < len(values) else None
    return above, below


def total(*terms):
    terms = [term for term in terms if term is not None]
    result = terms[0]
    for term in terms[1:]:
        result = result + term
    return result


def coefficients(rho, kmt, levels):
    zero = jnp.zeros_like(kmt[C])
    wet, lm, cell = [], [], []
    for d in range(5):
        w = [(kmt[d] > float(k)).astype(jnp.float32) for k in range(levels)]
        m = [w[k + 1] * w[k] for k in range(levels - 1)]
        st = [(rho[d][k + 1] - rho[d][k]) * m[k] for k in range(levels - 1)]
        wet.append(w)
        lm.append(m)
        cell.append([0.5 * total(*shift_sum(st, k)) for k in range(levels)])
    mask = [None] + [[wet[C][k] * wet[d][k] for k in range(levels)] for d in (E, W, N, S)]
    slope = [None]
    for d in (E, W, N, S):
        sign = 1.0 if d in (E, N) else -1.0
        slope.append(
            [
                taper(
                    sign
                    * (rho[d][k] - rho[C][k])
                    * mask[d][k]
                    / jnp.maximum(0.5 * (cell[d][k] + cell[C][k]), 1.0)
                )
                for k in range(levels)
            ]
        )
    cx = [0.5 * (slope[W][k] + slope[E][k]) for k in range(levels)]
    cy = [0.5 * (slope[S][k] + slope[N][k]) for k in range(levels)]
    xs, ys, zs = [], [], []
    for k in range(levels - 1):
        sxw = 0.5 * (cx[k] + cx[k + 1])
        syw = 0.5 * (cy[k] + cy[k + 1])
        xs.append(((REDI + SKEW) * 0.25) * sxw * lm[C][k])
        ys.append(((REDI + SKEW) * 0.25) * syw * lm[C][k])
        zs.append(REDI * (sxw * sxw + syw * syw) * lm[C][k])
    out = {}
    for k in range(levels):
        first, last = k == 0, k == levels - 1
        centre, up, down = 1.0, zero, zero
        q = zero
        for d in (E, W, N, S):
            sign = 1.0 if d in (E, N) else -1.0
            face = xs if d in (E, W) else ys
            p = (sign * (REDI - SKEW) * 0.25) * slope[d][k] * mask[d][k]
            q = q + p
            lo = zero if first else lm[d][k - 1]
            hi = zero if last else lm[d][k]
            flo = zero if first else face[k - 1]
            fhi = zero if last else face[k]
            own = sign * mask[d][k] * (fhi - flo)
            out[d, k, 1] = REDI * mask[d][k] + p * (lo - hi) + own
            out[d, k, 2] = zero if last else p * hi + sign * mask[d][k + 1] * fhi
            out[d, k, 0] = zero if first else -p * lo - sign * mask[d][k - 1] * flo
            centre = centre - REDI * mask[d][k] - own
            if not last:
                up = up - sign * mask[d][k + 1] * fhi
            if not first:
                down = down + sign * mask[d][k - 1] * flo
        lo = zero if first else lm[C][k - 1]
        hi = zero if last else lm[C][k]
        zlo = zero if first else zs[k - 1]
        zhi = zero if last else zs[k]
        out[C, k, 1] = centre + q * (lo - hi) - (zhi + zlo)
        out[C, k, 2] = up + q * hi + zhi
        out[C, k, 0] = down - q * lo + zlo
    return out


def kernel(
    sizes, x_ref, kmt_ref, out_ref,
    xv, kmt_own_ref, coef, edge, cols, west, east, north, south, from_n, from_s,
    load_sem, send_sem, recv_sem,
):
    tracers, levels, rows, lanes, n_lon, n_lat = sizes
    lon, lat = lax.axis_index("lon"), lax.axis_index("lat")
    at_top = lat == n_lat - 1
    below_top = jnp.logical_not(at_top)
    inner = lat > 0
    e_dev = (lax.rem(lon + 1, n_lon), lat)
    w_dev = (lax.rem(lon + n_lon - 1, n_lon), lat)
    fold_dev = (n_lon - 1 - lon, lat)
    plane = levels * rows
    per_reg = lanes // 2
    group = per_reg // levels
    pieces = tracers // group
    step = group * plane

    barrier = pltpu.get_barrier_semaphore()

    def greet(dev):
        pl.semaphore_signal(barrier, inc=1, device_id=dev, device_id_type=MESH)

    with jax.named_scope("greet"):

        @pl.when(at_top)
        def _():
            greet(fold_dev)

        @pl.when(below_top)
        def _():
            greet((lon, lat + 1))

        greet(e_dev)
        greet(w_dev)

        @pl.when(inner)
        def _():
            greet((lon, lat - 1))

    load_kmt = pltpu.make_async_copy(kmt_ref, kmt_own_ref, load_sem.at[pieces])
    load_kmt.start()
    loads = []
    for i in range(pieces):
        copy = pltpu.make_async_copy(
            x_ref.at[pl.ds(i * step, step)], xv.at[pl.ds(PAD + i * step, step)], load_sem.at[i]
        )
        copy.start()
        loads.append(copy)

    zeros = jnp.zeros((8, lanes), jnp.float32)
    xv[pl.ds(0, PAD), :] = zeros
    xv[pl.ds(PAD + tracers * plane, PAD), :] = zeros
    lane = lax.broadcasted_iota(jnp.int32, (8, lanes), 1)
    row = lax.broadcasted_iota(jnp.int32, (8, lanes), 0)
    even = lane % 2 == 0
    spot = (lane + 1) % lanes // 2
    backwards = lanes - 1 - lane
    from_east, from_west = lane == lanes - 1, lane == 0

    def flipped(value):
        return jnp.take_along_axis(value, backwards, axis=1)

    def pack_cols(i):
        acc = zeros
        for q in range(per_reg):
            value = xv[pl.ds(PAD + (i * per_reg + q) * rows, rows), :]
            if q:
                value = pltpu.roll(value, 2 * q, 1)
            acc = jnp.where(spot == q, value, acc)
        cols[pl.ds(8 + i * 8, 8), :] = acc

    def pack_rows(first, last):
        for t in range(first, last):
            base = PAD + t * plane
            n = xv[pl.ds(base + rows - 1, levels, stride=rows), :]
            north[pl.ds(HEAD + t * levels, levels), :] = n
            south[pl.ds(HEAD + t * levels, levels), :] = xv[pl.ds(base, levels, stride=rows), :]

    def turn_rows(first, count):
        @pl.when(at_top)
        def _():
            for i in range(first // 8, (first + count) // 8):
                north[pl.ds(i * 8, 8), :] = flipped(north[pl.ds(i * 8, 8), :])

    small = HEAD + 2 * levels
    big = (tracers - 2) * levels

    with jax.named_scope("pack0"):
        load_kmt.wait()
        kmt_own = kmt_own_ref[...].astype(jnp.float32)
        north[pl.ds(0, HEAD), :] = jnp.broadcast_to(kmt_own[rows - 1 : rows, :], (HEAD, lanes))
        south[pl.ds(0, HEAD), :] = jnp.broadcast_to(kmt_own[0:1, :], (HEAD, lanes))
        cols[pl.ds(0, 8), :] = kmt_own
        loads[0].wait()
        pack_rows(0, 2)
        turn_rows(0, small)
        pack_cols(0)

    with jax.named_scope("barrier"):

        @pl.when(inner)
        def _():
            pl.semaphore_wait(barrier, 4)

        @pl.when(jnp.logical_not(inner))
        def _():
            pl.semaphore_wait(barrier, 3)

    def send(src, dst, rows_at, count, s, dev, r=None):
        return pltpu.make_async_remote_copy(
            src_ref=src.at[pl.ds(rows_at, count)],
            dst_ref=dst.at[pl.ds(rows_at, count)],
            send_sem=send_sem.at[s],
            recv_sem=recv_sem.at[s if r is None else r],
            device_id=dev,
            device_id_type=MESH,
        )

    spans = ((0, small), (small, big))
    fold = [send(north, from_n, *spans[i], 2 + i, fold_dev, i) for i in range(2)]
    to_n = [send(north, from_s, *spans[i], 2 + i, (lon, lat + 1)) for i in range(2)]
    to_s = [send(south, from_n, *spans[i], i, (lon, lat - 1)) for i in range(2)]

    def columns(first, count, i):
        return (
            send(cols, west, first, count, 4 + 2 * i, e_dev),
            send(cols, east, first, count, 5 + 2 * i, w_dev),
        )

    def piece_columns(i):
        return columns(8 + i * 8, 8, i)

    def send_rows(part):
        @pl.when(at_top)
        def _():
            fold[part].start()

        @pl.when(below_top)
        def _():
            to_n[part].start()

        @pl.when(inner)
        def _():
            to_s[part].start()

    head_cols = columns(0, 16, 0)
    with jax.named_scope("send"):
        send_rows(0)
        for copy in head_cols:
            copy.start()
    with jax.named_scope("pack"):
        for i in range(1, pieces):
            loads[i].wait()
            pack_cols(i)
            for copy in piece_columns(i):
                copy.start()
        pack_rows(2, tracers)
        turn_rows(small, big)
        send_rows(1)

    with jax.named_scope("waitsmall"):

        @pl.when(jnp.logical_not(inner))
        def _():
            for i in range(small // 8):
                from_s[pl.ds(i * 8, 8), :] = zeros

        fold[0].wait_recv()

        @pl.when(inner)
        def _():
            to_n[0].wait_recv()

        for copy in head_cols:
            copy.wait_recv()

    def merged(at):
        return jnp.where(even, east[pl.ds(at, 8), :], pltpu.roll(west[pl.ds(at, 8), :], 2, 1))

    def beside(value, halo):
        e = jnp.where(from_east, halo, pltpu.roll(value, lanes - 1, 1))
        w = jnp.where(from_west, halo, pltpu.roll(value, 1, 1))
        return e, w

    def north_of(value, halo):
        return jnp.where(row == rows - 1, halo, pltpu.roll(value, rows - 1, 0))

    def south_of(value, halo):
        return jnp.where(row == 0, halo, pltpu.roll(value, 1, 0))

    with jax.named_scope("coefs"):
        rho = [[], [], [], [], []]
        rho_n = HALINE * from_n[pl.ds(HEAD + levels, levels), :] - THERMAL * from_n[pl.ds(HEAD, levels), :]
        rho_s = HALINE * from_s[pl.ds(HEAD + levels, levels), :] - THERMAL * from_s[pl.ds(HEAD, levels), :]
        reg = merged(8)
        rho_h = HALINE * pltpu.roll(reg, lanes - 2 * levels, 1) - THERMAL * reg
        for k in range(levels):
            own = HALINE * xv[pl.ds(PAD + plane + k * rows, rows), :] - THERMAL * xv[pl.ds(PAD + k * rows, rows), :]
            e, w = beside(own, pltpu.roll(rho_h, lanes - 2 * k - 1, 1))
            rho[C].append(own)
            rho[E].append(e)
            rho[W].append(w)
            rho[N].append(north_of(own, jnp.broadcast_to(rho_n[k : k + 1, :], (rows, lanes))))
            rho[S].append(south_of(own, jnp.broadcast_to(rho_s[k : k + 1, :], (rows, lanes))))
        kmts = [
            kmt_own,
            jnp.where(from_east, pltpu.roll(east[pl.ds(0, 8), :], lanes - 1, 1), pltpu.roll(kmt_own, lanes - 1, 1)),
            jnp.where(from_west, pltpu.roll(west[pl.ds(0, 8), :], 1, 1), pltpu.roll(kmt_own, 1, 1)),
            north_of(kmt_own, from_n[pl.ds(0, 8), :]),
            south_of(kmt_own, from_s[pl.ds(0, 8), :]),
        ]
        table = coefficients(rho, kmts, levels)
        for (d, k, dk), value in table.items():
            coef[pl.ds(((d * 3 + dk) * levels + k) * 8, 8), :] = value
        for slot, (d, at) in enumerate(((N, rows - 1), (S, 0))):
            for dk in range(3):
                place = pl.ds((d * 3 + dk) * plane + at, levels, stride=rows)
                edge[pl.ds((slot * 3 + dk) * 8, 8), :] = coef[place, :]
                coef[place, :] = zeros

    def piece(d, dk, k):
        return coef[pl.ds(((d * 3 + dk) * levels + k) * 8, 8), :]

    together = TOGETHER

    def batch(reg, i, first):
        fields = []
        for u in range(together):
            t = i * group + first + u
            base = pl.multiple_of(PAD + t * plane, 8)
            field = []
            for k in range(levels):
                own = xv[pl.ds(base + k * rows, rows), :]
                halo = pltpu.roll(reg, (2 * lanes - 2 * ((first + u) * levels + k) - 1) % lanes, 1)
                e, w = beside(own, halo)
                if UNALIGNED:
                    n = xv[pl.ds(base + k * rows + 1, rows), :]
                    s = xv[pl.ds(base + k * rows - 1, rows), :]
                else:
                    n = pltpu.roll(own, rows - 1, 0)
                    s = pltpu.roll(own, 1, 0)
                field.append((own, e, w, n, s))
            fields.append(field)
        for k in range(levels):
            sums = [None] * together
            for d in range(5):
                for dk in range(3):
                    if not 0 <= k + dk - 1 < levels:
                        continue
                    c = piece(d, dk, k)
                    for u in range(together):
                        term = c * fields[u][k + dk - 1][d]
                        sums[u] = term if sums[u] is None else sums[u] + term
            for u in range(together):
                t = i * group + first + u
                out_ref[pl.ds(pl.multiple_of(t * plane + k * rows, 8), rows), :] = sums[u]

    with jax.named_scope("main"):

        @pl.loop(0, pieces)
        def _(i):
            @pl.when(i > 0)
            def _():
                for copy in piece_columns(i):
                    copy.wait_recv()

            reg = merged(pl.multiple_of(8 + i * 8, 8))
            for first in range(0, group, together):
                batch(reg, i, first)

    def fix(slot, source, at):
        cs = [edge[pl.ds((slot * 3 + dk) * 8, 8), :] for dk in range(3)]

        @pl.loop(0, pieces)
        def _(i):
            for u in range(group):
                t = i * group + u
                h = source[pl.ds(pl.multiple_of(HEAD + t * levels, 8), levels), :]
                add = cs[1] * h + cs[2] * pltpu.roll(h, levels - 1, 0) + cs[0] * pltpu.roll(h, 1, 0)
                place = pl.ds(t * plane + at, levels, stride=rows)
                out_ref[place, :] = out_ref[place, :] + add

    with jax.named_scope("fixs"):

        @pl.when(inner)
        def _():
            to_n[1].wait_recv()
            fix(1, from_s, 0)

    with jax.named_scope("waitbig"):
        fold[1].wait_recv()
    with jax.named_scope("fixn"):
        fix(0, from_n, rows - 1)

    with jax.named_scope("end"):
        for part in range(2):
            fold[part].wait_send()

            @pl.when(inner)
            def _():
                to_s[part].wait_send()

        for copy in head_cols:
            copy.wait_send()
        for i in range(1, pieces):
            for copy in piece_columns(i):
                copy.wait_send()


def solution(mesh):
    n_lon, n_lat = mesh.shape["lon"], mesh.shape["lat"]

    def local(tracers, kmt):
        nt, levels, rows, lanes = tracers.shape
        flat = tracers.reshape(nt * levels * rows, lanes)
        total_rows = nt * levels * rows
        pieces = nt * levels * 2 // lanes
        packed = (pieces + 1) * 8
        halo = HEAD + nt * levels

        def vmem(*shape):
            return pltpu.VMEM(shape, jnp.float32)

        out = pl.pallas_call(
            functools.partial(kernel, (nt, levels, rows, lanes, n_lon, n_lat)),
            out_shape=pltpu.VMEM((total_rows, lanes), jnp.float32),
            in_specs=[pl.BlockSpec(memory_space=pltpu.HBM), pl.BlockSpec(memory_space=pltpu.HBM)],
            out_specs=pl.BlockSpec(memory_space=pltpu.VMEM),
            scratch_shapes=[
                vmem(total_rows + 2 * PAD, lanes),
                pltpu.VMEM((rows, lanes), jnp.int32),
                vmem(15 * levels * 8, lanes),
                vmem(6 * 8, lanes),
                vmem(packed, lanes),
                vmem(packed, lanes),
                vmem(packed, lanes),
                vmem(halo, lanes),
                vmem(halo, lanes),
                vmem(halo, lanes),
                vmem(halo, lanes),
                pltpu.SemaphoreType.DMA((pieces + 1,)),
                pltpu.SemaphoreType.DMA((4 + 2 * pieces,)),
                pltpu.SemaphoreType.DMA((4 + 2 * pieces,)),
            ],
            compiler_params=pltpu.CompilerParams(collective_id=0, has_side_effects=True),
        )(flat, kmt)
        return out.reshape(nt, levels, rows, lanes)

    return jax.shard_map(
        local,
        mesh=mesh,
        in_specs=(P(None, None, "lat", "lon"), P("lat", "lon")),
        out_specs=P(None, None, "lat", "lon"),
        check_vma=False,
    )
```

```python
import functools

import jax
import jax.numpy as jnp
from jax import lax
from jax.experimental import pallas as pl
from jax.experimental.pallas import tpu as pltpu
from jax.sharding import PartitionSpec as P

THERMAL = 0.2
HALINE = 0.8
REDI = 0.1
SKEW = 0.05
SLOPE_MAX = 0.6
SLOPE_WIDTH = 0.2

MESH = pl.DeviceIdType.MESH
PAD = 8
HEAD = 8
TOGETHER = 2
UNALIGNED = False
C, E, W, N, S = range(5)


def taper(slope):
    return slope * 0.5 * (1.0 + jnp.tanh((SLOPE_MAX - jnp.abs(slope)) / SLOPE_WIDTH))


def shift_sum(values, k):
    above = values[k - 1] if k > 0 else None
    below = values[k] if k < len(values) else None
    return above, below


def total(*terms):
    terms = [term for term in terms if term is not None]
    result = terms[0]
    for term in terms[1:]:
        result = result + term
    return result


def coefficients(rho, kmt, levels):
    zero = jnp.zeros_like(kmt[C])
    wet, lm, cell = [], [], []
    for d in range(5):
        w = [(kmt[d] > float(k)).astype(jnp.float32) for k in range(levels)]
        m = [w[k + 1] * w[k] for k in range(levels - 1)]
        st = [(rho[d][k + 1] - rho[d][k]) * m[k] for k in range(levels - 1)]
        wet.append(w)
        lm.append(m)
        cell.append([0.5 * total(*shift_sum(st, k)) for k in range(levels)])
    mask = [None] + [[wet[C][k] * wet[d][k] for k in range(levels)] for d in (E, W, N, S)]
    slope = [None]
    for d in (E, W, N, S):
        sign = 1.0 if d in (E, N) else -1.0
        slope.append(
            [
                taper(
                    sign
                    * (rho[d][k] - rho[C][k])
                    * mask[d][k]
                    / jnp.maximum(0.5 * (cell[d][k] + cell[C][k]), 1.0)
                )
                for k in range(levels)
            ]
        )
    cx = [0.5 * (slope[W][k] + slope[E][k]) for k in range(levels)]
    cy = [0.5 * (slope[S][k] + slope[N][k]) for k in range(levels)]
    xs, ys, zs = [], [], []
    for k in range(levels - 1):
        sxw = 0.5 * (cx[k] + cx[k + 1])
        syw = 0.5 * (cy[k] + cy[k + 1])
        xs.append(((REDI + SKEW) * 0.25) * sxw * lm[C][k])
        ys.append(((REDI + SKEW) * 0.25) * syw * lm[C][k])
        zs.append(REDI * (sxw * sxw + syw * syw) * lm[C][k])
    out = {}
    for k in range(levels):
        first, last = k == 0, k == levels - 1
        centre, up, down = 1.0, zero, zero
        q = zero
        for d in (E, W, N, S):
            sign = 1.0 if d in (E, N) else -1.0
            face = xs if d in (E, W) else ys
            p = (sign * (REDI - SKEW) * 0.25) * slope[d][k] * mask[d][k]
            q = q + p
            lo = zero if first else lm[d][k - 1]
            hi = zero if last else lm[d][k]
            flo = zero if first else face[k - 1]
            fhi = zero if last else face[k]
            own = sign * mask[d][k] * (fhi - flo)
            out[d, k, 1] = REDI * mask[d][k] + p * (lo - hi) + own
            out[d, k, 2] = zero if last else p * hi + sign * mask[d][k + 1] * fhi
            out[d, k, 0] = zero if first else -p * lo - sign * mask[d][k - 1] * flo
            centre = centre - REDI * mask[d][k] - own
            if not last:
                up = up - sign * mask[d][k + 1] * fhi
            if not first:
                down = down + sign * mask[d][k - 1] * flo
        lo = zero if first else lm[C][k - 1]
        hi = zero if last else lm[C][k]
        zlo = zero if first else zs[k - 1]
        zhi = zero if last else zs[k]
        out[C, k, 1] = centre + q * (lo - hi) - (zhi + zlo)
        out[C, k, 2] = up + q * hi + zhi
        out[C, k, 0] = down - q * lo + zlo
    return out


def kernel(
    sizes, x_ref, kmt_ref, out_ref,
    xv, kmt_own_ref, coef, edge, cols, west, east, north, south, from_n, from_s,
    load_sem, send_sem, recv_sem,
):
    tracers, levels, rows, lanes, n_lon, n_lat = sizes
    lon, lat = lax.axis_index("lon"), lax.axis_index("lat")
    at_top = lat == n_lat - 1
    below_top = jnp.logical_not(at_top)
    inner = lat > 0
    e_dev = (lax.rem(lon + 1, n_lon), lat)
    w_dev = (lax.rem(lon + n_lon - 1, n_lon), lat)
    fold_dev = (n_lon - 1 - lon, lat)
    plane = levels * rows
    per_reg = lanes // 2
    group = per_reg // levels
    pieces = tracers // group
    step = group * plane

    barrier = pltpu.get_barrier_semaphore()

    def greet(dev):
        pl.semaphore_signal(barrier, inc=1, device_id=dev, device_id_type=MESH)

    with jax.named_scope("greet"):

        @pl.when(at_top)
        def _():
            greet(fold_dev)

        @pl.when(below_top)
        def _():
            greet((lon, lat + 1))

        greet(e_dev)
        greet(w_dev)

        @pl.when(inner)
        def _():
            greet((lon, lat - 1))

    load_kmt = pltpu.make_async_copy(kmt_ref, kmt_own_ref, load_sem.at[pieces + 1])
    load_kmt.start()
    loads = []
    cuts = [0, 2 * plane] + [i * step for i in range(1, pieces + 1)]
    for i, (first, last) in enumerate(zip(cuts, cuts[1:])):
        copy = pltpu.make_async_copy(
            x_ref.at[pl.ds(first, last - first)], xv.at[pl.ds(PAD + first, last - first)], load_sem.at[i]
        )
        copy.start()
        loads.append(copy)

    zeros = jnp.zeros((8, lanes), jnp.float32)
    xv[pl.ds(0, PAD), :] = zeros
    xv[pl.ds(PAD + tracers * plane, PAD), :] = zeros
    lane = lax.broadcasted_iota(jnp.int32, (8, lanes), 1)
    row = lax.broadcasted_iota(jnp.int32, (8, lanes), 0)
    even = lane % 2 == 0
    spot = (lane + 1) % lanes // 2
    backwards = lanes - 1 - lane
    from_east, from_west = lane == lanes - 1, lane == 0

    def flipped(value):
        return jnp.take_along_axis(value, backwards, axis=1)

    def pack_cols(i, count, to):
        acc = zeros
        for q in range(count):
            value = xv[pl.ds(PAD + (i * per_reg + q) * rows, rows), :]
            if q:
                value = pltpu.roll(value, 2 * q, 1)
            acc = jnp.where(spot == q, value, acc)
        cols[pl.ds(to, 8), :] = acc

    def pack_rows(first, last):
        for t in range(first, last):
            base = PAD + t * plane
            n = xv[pl.ds(base + rows - 1, levels, stride=rows), :]
            north[pl.ds(HEAD + t * levels, levels), :] = n
            south[pl.ds(HEAD + t * levels, levels), :] = xv[pl.ds(base, levels, stride=rows), :]

    def turn_rows(first, count):
        @pl.when(at_top)
        def _():
            for i in range(first // 8, (first + count) // 8):
                north[pl.ds(i * 8, 8), :] = flipped(north[pl.ds(i * 8, 8), :])

    small = HEAD + 2 * levels
    big = (tracers - 2) * levels

    with jax.named_scope("pack0"):
        load_kmt.wait()
        kmt_own = kmt_own_ref[...].astype(jnp.float32)
        north[pl.ds(0, HEAD), :] = jnp.broadcast_to(kmt_own[rows - 1 : rows, :], (HEAD, lanes))
        south[pl.ds(0, HEAD), :] = jnp.broadcast_to(kmt_own[0:1, :], (HEAD, lanes))
        cols[pl.ds(0, 8), :] = kmt_own
        loads[0].wait()
        pack_rows(0, 2)
        turn_rows(0, small)
        pack_cols(0, 2 * levels, 8)

    with jax.named_scope("barrier"):

        @pl.when(inner)
        def _():
            pl.semaphore_wait(barrier, 4)

        @pl.when(jnp.logical_not(inner))
        def _():
            pl.semaphore_wait(barrier, 3)

    def send(src, dst, rows_at, count, s, dev, r=None):
        return pltpu.make_async_remote_copy(
            src_ref=src.at[pl.ds(rows_at, count)],
            dst_ref=dst.at[pl.ds(rows_at, count)],
            send_sem=send_sem.at[s],
            recv_sem=recv_sem.at[s if r is None else r],
            device_id=dev,
            device_id_type=MESH,
        )

    spans = ((0, small), (small, big))
    fold = [send(north, from_n, *spans[i], 2 + i, fold_dev, i) for i in range(2)]
    to_n = [send(north, from_s, *spans[i], 2 + i, (lon, lat + 1)) for i in range(2)]
    to_s = [send(south, from_n, *spans[i], i, (lon, lat - 1)) for i in range(2)]

    def columns(first, count, i):
        return (
            send(cols, west, first, count, 4 + 2 * i, e_dev),
            send(cols, east, first, count, 5 + 2 * i, w_dev),
        )

    def piece_columns(i):
        return columns(16 + i * 8, 8, 1 + i)

    def send_rows(part):
        @pl.when(at_top)
        def _():
            fold[part].start()

        @pl.when(below_top)
        def _():
            to_n[part].start()

        @pl.when(inner)
        def _():
            to_s[part].start()

    head_cols = columns(0, 16, 0)
    with jax.named_scope("send"):
        send_rows(0)
        for copy in head_cols:
            copy.start()
    with jax.named_scope("pack"):
        for i in range(pieces):
            loads[1 + i].wait()
            pack_cols(i, per_reg, 16 + i * 8)
            for copy in piece_columns(i):
                copy.start()
        pack_rows(2, tracers)
        turn_rows(small, big)
        send_rows(1)

    with jax.named_scope("waitsmall"):

        @pl.when(jnp.logical_not(inner))
        def _():
            for i in range(small // 8):
                from_s[pl.ds(i * 8, 8), :] = zeros

        fold[0].wait_recv()

        @pl.when(inner)
        def _():
            to_n[0].wait_recv()

        for copy in head_cols:
            copy.wait_recv()

    def merged(at):
        return jnp.where(even, east[pl.ds(at, 8), :], pltpu.roll(west[pl.ds(at, 8), :], 2, 1))

    def beside(value, halo):
        e = jnp.where(from_east, halo, pltpu.roll(value, lanes - 1, 1))
        w = jnp.where(from_west, halo, pltpu.roll(value, 1, 1))
        return e, w

    def north_of(value, halo):
        return jnp.where(row == rows - 1, halo, pltpu.roll(value, rows - 1, 0))

    def south_of(value, halo):
        return jnp.where(row == 0, halo, pltpu.roll(value, 1, 0))

    with jax.named_scope("coefs"):
        rho = [[], [], [], [], []]
        rho_n = HALINE * from_n[pl.ds(HEAD + levels, levels), :] - THERMAL * from_n[pl.ds(HEAD, levels), :]
        rho_s = HALINE * from_s[pl.ds(HEAD + levels, levels), :] - THERMAL * from_s[pl.ds(HEAD, levels), :]
        reg = merged(8)
        rho_h = HALINE * pltpu.roll(reg, lanes - 2 * levels, 1) - THERMAL * reg
        for k in range(levels):
            own = HALINE * xv[pl.ds(PAD + plane + k * rows, rows), :] - THERMAL * xv[pl.ds(PAD + k * rows, rows), :]
            e, w = beside(own, pltpu.roll(rho_h, lanes - 2 * k - 1, 1))
            rho[C].append(own)
            rho[E].append(e)
            rho[W].append(w)
            rho[N].append(north_of(own, jnp.broadcast_to(rho_n[k : k + 1, :], (rows, lanes))))
            rho[S].append(south_of(own, jnp.broadcast_to(rho_s[k : k + 1, :], (rows, lanes))))
        kmts = [
            kmt_own,
            jnp.where(from_east, pltpu.roll(east[pl.ds(0, 8), :], lanes - 1, 1), pltpu.roll(kmt_own, lanes - 1, 1)),
            jnp.where(from_west, pltpu.roll(west[pl.ds(0, 8), :], 1, 1), pltpu.roll(kmt_own, 1, 1)),
            north_of(kmt_own, from_n[pl.ds(0, 8), :]),
            south_of(kmt_own, from_s[pl.ds(0, 8), :]),
        ]
        table = coefficients(rho, kmts, levels)
        for (d, k, dk), value in table.items():
            coef[pl.ds(((d * 3 + dk) * levels + k) * 8, 8), :] = value
        for slot, (d, at) in enumerate(((N, rows - 1), (S, 0))):
            for dk in range(3):
                place = pl.ds((d * 3 + dk) * plane + at, levels, stride=rows)
                edge[pl.ds((slot * 3 + dk) * 8, 8), :] = coef[place, :]
                coef[place, :] = zeros

    def piece(d, dk, k):
        return coef[pl.ds(((d * 3 + dk) * levels + k) * 8, 8), :]

    together = TOGETHER

    def batch(reg, i, first):
        fields = []
        for u in range(together):
            t = i * group + first + u
            base = pl.multiple_of(PAD + t * plane, 8)
            field = []
            for k in range(levels):
                own = xv[pl.ds(base + k * rows, rows), :]
                halo = pltpu.roll(reg, (2 * lanes - 2 * ((first + u) * levels + k) - 1) % lanes, 1)
                e, w = beside(own, halo)
                if UNALIGNED:
                    n = xv[pl.ds(base + k * rows + 1, rows), :]
                    s = xv[pl.ds(base + k * rows - 1, rows), :]
                else:
                    n = pltpu.roll(own, rows - 1, 0)
                    s = pltpu.roll(own, 1, 0)
                field.append((own, e, w, n, s))
            fields.append(field)
        for k in range(levels):
            sums = [None] * together
            for d in range(5):
                for dk in range(3):
                    if not 0 <= k + dk - 1 < levels:
                        continue
                    c = piece(d, dk, k)
                    for u in range(together):
                        term = c * fields[u][k + dk - 1][d]
                        sums[u] = term if sums[u] is None else sums[u] + term
            for u in range(together):
                t = i * group + first + u
                out_ref[pl.ds(pl.multiple_of(t * plane + k * rows, 8), rows), :] = sums[u]

    with jax.named_scope("main"):

        @pl.loop(0, pieces)
        def _(i):
            for copy in piece_columns(i):
                copy.wait_recv()
            reg = merged(pl.multiple_of(16 + i * 8, 8))
            for first in range(0, group, together):
                batch(reg, i, first)

    def fix(slot, source, at):
        cs = [edge[pl.ds((slot * 3 + dk) * 8, 8), :] for dk in range(3)]

        @pl.loop(0, pieces)
        def _(i):
            for u in range(group):
                t = i * group + u
                h = source[pl.ds(pl.multiple_of(HEAD + t * levels, 8), levels), :]
                add = cs[1] * h + cs[2] * pltpu.roll(h, levels - 1, 0) + cs[0] * pltpu.roll(h, 1, 0)
                place = pl.ds(t * plane + at, levels, stride=rows)
                out_ref[place, :] = out_ref[place, :] + add

    with jax.named_scope("fixs"):

        @pl.when(inner)
        def _():
            to_n[1].wait_recv()
            fix(1, from_s, 0)

    with jax.named_scope("waitbig"):
        fold[1].wait_recv()
    with jax.named_scope("fixn"):
        fix(0, from_n, rows - 1)

    with jax.named_scope("end"):
        for part in range(2):
            fold[part].wait_send()

            @pl.when(inner)
            def _():
                to_s[part].wait_send()

        for copy in head_cols:
            copy.wait_send()
        for i in range(pieces):
            for copy in piece_columns(i):
                copy.wait_send()


def solution(mesh):
    n_lon, n_lat = mesh.shape["lon"], mesh.shape["lat"]

    def local(tracers, kmt):
        nt, levels, rows, lanes = tracers.shape
        flat = tracers.reshape(nt * levels * rows, lanes)
        total_rows = nt * levels * rows
        pieces = nt * levels * 2 // lanes
        packed = (pieces + 2) * 8
        halo = HEAD + nt * levels

        def vmem(*shape):
            return pltpu.VMEM(shape, jnp.float32)

        out = pl.pallas_call(
            functools.partial(kernel, (nt, levels, rows, lanes, n_lon, n_lat)),
            out_shape=pltpu.VMEM((total_rows, lanes), jnp.float32),
            in_specs=[pl.BlockSpec(memory_space=pltpu.HBM), pl.BlockSpec(memory_space=pltpu.HBM)],
            out_specs=pl.BlockSpec(memory_space=pltpu.VMEM),
            scratch_shapes=[
                vmem(total_rows + 2 * PAD, lanes),
                pltpu.VMEM((rows, lanes), jnp.int32),
                vmem(15 * levels * 8, lanes),
                vmem(6 * 8, lanes),
                vmem(packed, lanes),
                vmem(packed, lanes),
                vmem(packed, lanes),
                vmem(halo, lanes),
                vmem(halo, lanes),
                vmem(halo, lanes),
                vmem(halo, lanes),
                pltpu.SemaphoreType.DMA((pieces + 2,)),
                pltpu.SemaphoreType.DMA((6 + 2 * pieces,)),
                pltpu.SemaphoreType.DMA((6 + 2 * pieces,)),
            ],
            compiler_params=pltpu.CompilerParams(collective_id=0, has_side_effects=True),
        )(flat, kmt)
        return out.reshape(nt, levels, rows, lanes)

    return jax.shard_map(
        local,
        mesh=mesh,
        in_specs=(P(None, None, "lat", "lon"), P("lat", "lon")),
        out_specs=P(None, None, "lat", "lon"),
        check_vma=False,
    )
```
